16 devices in a mesh: dp: 1, sp: 16 (over x, y, z, core).
Axes of the slice: x: 2, y: 2, z: 2, core: 2. Of those that a mesh axis runs over, the one named last changes fastest.
Arguments:
- q: bfloat16 [32, 32, 64], P('dp')
- k: bfloat16 [32, 8192, 32, 64], P('dp', 'sp')
- v: bfloat16 [32, 8192, 32, 64], P('dp', 'sp')
Outputs:
- q: bfloat16 [32, 32, 64], P('dp')
All inputs are finite; a program needn't handle non-finite values.
Results may differ from the reference program's by a relative error of at most 0.012.
Values are sent between devices in bfloat16 or wider.
A program may use at most 2 GiB of HBM per device.

```python
import jax
import jax.numpy as jnp

BATCH = 32
CACHE = 8192
HEADS = 32
KV_HEADS = 32
HEAD = 64


def setup_inputs(seed: int = 0, part: int = 0) -> dict:
    kq, kk, kv = (jax.random.fold_in(k, part) for k in jax.random.split(jax.random.key(seed), 3))
    return {
        "q": (3 * jax.random.normal(kq, (BATCH, HEADS, HEAD), jnp.float32)).astype(jnp.bfloat16),
        "k": jax.random.normal(kk, (BATCH, CACHE, KV_HEADS, HEAD), jnp.float32).astype(jnp.bfloat16),
        "v": jax.random.normal(kv, (BATCH, CACHE, KV_HEADS, HEAD), jnp.float32).astype(jnp.bfloat16),
    }


def einsum(form, a, b):
    return jnp.einsum(form, a.astype(jnp.float32), b.astype(jnp.float32))


def reference(q, k, v):
    grouped = q.reshape(BATCH, KV_HEADS, -1, HEAD)
    scores = einsum("bgsd,bugd->bgsu", grouped, k) * HEAD**-0.5
    weights = jax.nn.softmax(scores, -1).astype(jnp.bfloat16)
    return einsum("bgsu,bugd->bgsd", weights, v).astype(jnp.bfloat16).reshape(BATCH, HEADS, HEAD)
```

```python
import jax
import jax.numpy as jnp
from jax import lax
from jax.experimental import pallas as pl
from jax.experimental.pallas import tpu as pltpu
from jax.sharding import PartitionSpec as P

MESH = pl.DeviceIdType.MESH
BF16, F32 = jnp.bfloat16, jnp.float32

DEV = 16
SEQ = 32
HEADS = 32
HEAD = 64
RUN = 512
HALF = 16
ROWS = HALF * HEAD
GROUP = 4
GROUPS = SEQ // GROUP
LAG = 8
AHEAD = LAG // GROUP
SLOTS = 8


def peers(me):
    bits = [(me // 2**i) % 2 for i in range(4)]
    for flip in (14, 15, 12, 10, 6, 13, 11, 7, 8, 4, 2, 9, 5, 3, 1):
        yield sum((1 - bit if flip >> i & 1 else bit) * 2**i for i, bit in enumerate(bits))


def kernel(q_ref, k_ref, v_ref, out_ref, kbuf, vbuf, ebuf, stats, parts, ksem, vsem, stat_send, stat_recv, part_send, part_recv):
    me = lax.axis_index("sp")
    row = lax.broadcasted_iota(jnp.int32, (HALF, 128), 0)
    lane = lax.broadcasted_iota(jnp.int32, (HALF, 128), 1)

    def k_copy(b, slot):
        return pltpu.make_async_copy(k_ref.at[b], kbuf.at[slot], ksem.at[slot])

    def v_copy(b, slot):
        return pltpu.make_async_copy(v_ref.at[b], vbuf.at[slot], vsem.at[slot])

    def send(ref, send_sem, recv_sem):
        for peer in peers(me):
            pltpu.make_async_remote_copy(ref, ref, send_sem, recv_sem, device_id={"sp": peer}, device_id_type=MESH).start()

    def wait_peers(ref, sem):
        some = ref.at[pl.ds(0, DEV - 1)]
        pltpu.make_async_copy(some, some, sem).wait()

    def scores(b, slot, i, rows):
        highs, sums = rows
        k_copy(b, slot).wait()
        for g in range(2):
            query = q_ref[b, HALF * g : HALF * (g + 1), :].astype(F32)
            query = jnp.concatenate([query, query], -1)
            query = jnp.where(lane // HEAD == row % 2, query, 0.0)
            query = jnp.concatenate([jnp.where(row // 2 == c, query, 0.0).astype(BF16) for c in range(HALF // 2)], -1)
            score = jnp.dot(query, kbuf[slot, ROWS * g : ROWS * (g + 1), :], preferred_element_type=F32) * HEAD**-0.5
            high = jnp.max(score, -1, keepdims=True)
            weight = jnp.exp(score - high)
            ebuf[b, g] = weight
            here = lane // HALF == 2 * i + g
            highs = jnp.where(here, high, highs)
            sums = jnp.where(here, jnp.sum(weight, -1, keepdims=True), sums)
        return highs, sums

    def exchange(g, rows):
        mine = lane % HALF == row
        for i, x in enumerate(rows):
            stats[g, me, :, 128 * i : 128 * (i + 1)] = jnp.sum(jnp.where(mine, x, 0.0), 0, keepdims=True)
        send(stats.at[g, me], stat_send.at[g], stat_recv.at[g])

    def shares(g):
        wait_peers(stats.at[g], stat_recv.at[g])
        high = stats[g, :, :, 0:128]
        top = jnp.max(high, 0)
        total = jnp.sum(stats[g, :, :, 128:256] * jnp.exp(high - top[None]), 0)
        return jnp.exp(stats[g, me, :, 0:128] - top) / total

    def values(b, slot, i, share):
        v_copy(b, slot).wait()
        halves = []
        for g in range(2):
            scale = jnp.sum(jnp.where(lane == HALF * (2 * i + g) + row, share, 0.0), -1, keepdims=True)
            weight = (ebuf[b, g] * scale).astype(BF16)
            seen = jnp.zeros((HALF, 128), F32)
            for c in range(0, HALF // 2, 2):
                first = ROWS * g + 128 * c
                wide = lax.dot_general(weight, vbuf[slot, first : first + 256, :], (((1,), (1,)), ((), ())), preferred_element_type=F32)
                seen = jnp.where(row // 2 == c, wide[:, :128], seen)
                seen = jnp.where(row // 2 == c + 1, wide[:, 128:], seen)
            halves.append(jnp.where(row % 2 == g, seen, pltpu.roll(seen, HEAD, 1)))
        parts[b, me] = jnp.where(lane < HEAD, *halves).astype(BF16)
        send(parts.at[b, me], part_send.at[b], part_recv.at[b])

    def finish(b):
        wait_peers(parts.at[b], part_recv.at[b])
        total = jnp.sum(parts[b].astype(F32), 0)
        out_ref[b, 0:HALF, :] = total[:, :HEAD].astype(BF16)
        out_ref[b, HALF:HEADS, :] = pltpu.roll(total, HEAD, 1)[:, :HEAD].astype(BF16)

    barrier = pltpu.get_barrier_semaphore()
    for b in range(SLOTS):
        k_copy(b, b).start()
    for peer in peers(me):
        pl.semaphore_signal(barrier, inc=1, device_id={"sp": peer}, device_id_type=MESH)

    empty = (jnp.zeros((HALF, 128), F32),) * 2

    def head(g, _):
        rows = empty
        for i in range(GROUP):
            b = GROUP * g + i
            rows = scores(b, b, i, rows)
            k_copy(b + SLOTS, b).start()
            v_copy(b, b).start()

        @pl.when(g == 0)
        def _():
            pl.semaphore_wait(barrier, DEV - 1)

        exchange(g, rows)
        return 0

    lax.fori_loop(0, AHEAD, head, 0)

    def body(g, _):
        share = shares(g)
        rows = empty
        for i in range(GROUP):
            b = GROUP * g + i
            slot = b % SLOTS
            rows = scores(b + LAG, slot, i, rows)
            values(b, slot, i, share)
        exchange(g + AHEAD, rows)
        for i in range(GROUP):
            b = GROUP * g + i
            slot = b % SLOTS
            v_copy(b + SLOTS, slot).start()

            @pl.when(b + LAG + SLOTS < SEQ)
            def _():
                k_copy(b + LAG + SLOTS, slot).start()

        @pl.when(g >= 2)
        def _():
            for i in range(GROUP):
                finish(GROUP * (g - 2) + i)

        return 0

    lax.fori_loop(0, GROUPS - AHEAD, body, 0)

    def tail(g, _):
        share = shares(g)
        for i in range(GROUP):
            b = GROUP * g + i
            values(b, b % SLOTS, i, share)
        return 0

    lax.fori_loop(GROUPS - AHEAD, GROUPS, tail, 0)

    def last(b, _):
        finish(b)
        return 0

    lax.fori_loop(GROUP * (GROUPS - AHEAD - 2), SEQ, last, 0)

    def drain(b, _):
        wait_peers(parts.at[b], part_send.at[b])
        return 0

    lax.fori_loop(0, SEQ, drain, 0)
    for g in range(GROUPS):
        wait_peers(stats.at[g], stat_send.at[g])


def solution(mesh):
    def step(q, k, v):
        k, v = (x.transpose(0, 2, 3, 1).reshape(SEQ, HEADS * HEAD, RUN) for x in (k, v))
        return pl.pallas_call(
            kernel,
            out_shape=jax.ShapeDtypeStruct(q.shape, BF16),
            in_specs=[pl.BlockSpec(memory_space=pltpu.VMEM)] + [pl.BlockSpec(memory_space=pl.ANY)] * 2,
            out_specs=pl.BlockSpec(memory_space=pltpu.VMEM),
            scratch_shapes=[
                pltpu.VMEM((SLOTS, HEADS * HEAD, RUN), BF16),
                pltpu.VMEM((SLOTS, HEADS * HEAD, RUN), BF16),
                pltpu.VMEM((SEQ, 2, HALF, RUN), F32),
                pltpu.VMEM((GROUPS, DEV, 1, 256), F32),
                pltpu.VMEM((SEQ, DEV, HALF, 128), BF16),
                pltpu.SemaphoreType.DMA((SLOTS,)),
                pltpu.SemaphoreType.DMA((SLOTS,)),
                pltpu.SemaphoreType.DMA((GROUPS,)),
                pltpu.SemaphoreType.DMA((GROUPS,)),
                pltpu.SemaphoreType.DMA((SEQ,)),
                pltpu.SemaphoreType.DMA((SEQ,)),
            ],
            compiler_params=pltpu.CompilerParams(collective_id=0, has_side_effects=True, vmem_limit_bytes=50 * 2**20),
            name="attend",
        )(q, k, v)

    return jax.shard_map(
        step,
        mesh=mesh,
        in_specs=(P("dp", None, None), P("dp", "sp", None, None), P("dp", "sp", None, None)),
        out_specs=P("dp", None, None),
        check_vma=False,
    )
```

```python
import jax
import jax.numpy as jnp
from jax import lax
from jax.experimental import pallas as pl
from jax.experimental.pallas import tpu as pltpu
from jax.sharding import PartitionSpec as P

MESH = pl.DeviceIdType.MESH
BF16, F32 = jnp.bfloat16, jnp.float32

DEV = 16
SEQ = 32
PAIRS = SEQ // 2
HEADS = 32
HEAD = 64
RUN = 512
HALF = 16
ROWS = HALF * HEAD
LAG = 3
AHEAD = 2
SLOTS = 2 * (AHEAD + 1)
BUNCH = 4
BUNCHES = 3
DIRECT = PAIRS - BUNCH * BUNCHES
RAW = 3


def peers(me):
    bits = [(me // 2**i) % 2 for i in range(4)]
    for flip in (14, 15, 12, 10, 6, 13, 11, 7, 8, 4, 2, 9, 5, 3, 1):
        yield sum((1 - bit if flip >> i & 1 else bit) * 2**i for i, bit in enumerate(bits))


def kernel(q_ref, k_ref, v_ref, out_ref, qbuf, kbuf, vbuf, weights, raw, stats, cut, came, summed, parts, qsem, ksem, vsem, stat_send, stat_recv, cut_send, cut_recv, sum_send, sum_recv, part_send, part_recv):
    me = lax.axis_index("sp")
    row = lax.broadcasted_iota(jnp.int32, (HALF, 128), 0)
    lane = lax.broadcasted_iota(jnp.int32, (HALF, 128), 1)

    def k_copy(b):
        return pltpu.make_async_copy(k_ref.at[b], kbuf.at[b % SLOTS], ksem.at[b % SLOTS])

    def v_copy(b):
        return pltpu.make_async_copy(v_ref.at[b], vbuf.at[b % SLOTS], vsem.at[b % SLOTS])

    def start(copy, p):
        for i in range(2):
            copy(2 * p + i).start()

    def wait(copy, p):
        for i in range(2):
            copy(2 * p + i).wait()

    def send(ref, send_sem, recv_sem):
        for peer in peers(me):
            pltpu.make_async_remote_copy(ref, ref, send_sem, recv_sem, device_id={"sp": peer}, device_id_type=MESH).start()

    def wait_peers(ref, sem):
        some = ref.at[pl.ds(0, DEV - 1)]
        pltpu.make_async_copy(some, some, sem).wait()

    def scores(p):
        highs = sums = jnp.zeros((HALF, 128), F32)
        for i in range(2):
            b = 2 * p + i
            for g in range(2):
                query = qbuf[b, HALF * g : HALF * (g + 1), :].astype(F32)
                query = jnp.concatenate([query, query], -1)
                query = jnp.where(lane // HEAD == row % 2, query, 0.0)
                query = jnp.concatenate([jnp.where(row // 2 == c, query, 0.0).astype(BF16) for c in range(HALF // 2)], -1)
                score = jnp.dot(query, kbuf[b % SLOTS, ROWS * g : ROWS * (g + 1), :], preferred_element_type=F32) * HEAD**-0.5
                high = jnp.max(score, -1, keepdims=True)
                weight = jnp.exp(score - high)
                weights[b, g] = weight.astype(BF16)
                here = lane // HALF == 2 * i + g
                highs = jnp.where(here, high, highs)
                sums = jnp.where(here, jnp.sum(weight, -1, keepdims=True), sums)
        mine = lane % HALF == row
        stats[p, me, :, 0:128] = jnp.sum(jnp.where(mine, highs, 0.0), 0, keepdims=True)
        stats[p, me, :, 128:256] = jnp.sum(jnp.where(mine, sums, 0.0), 0, keepdims=True)

    def send_stats(p):
        send(stats.at[p, me], stat_send.at[p], stat_recv.at[p])

    def wait_stats(p):
        wait_peers(stats.at[p], stat_recv.at[p])

    def values(p, i):
        b = 2 * p + i
        for g in range(2):
            seen = jnp.zeros((HALF, 128), F32)
            for c in range(0, HALF // 2, 2):
                first = ROWS * g + 128 * c
                wide = lax.dot_general(weights[b, g], vbuf[b % SLOTS, first : first + 256, :], (((1,), (1,)), ((), ())), preferred_element_type=F32)
                seen = jnp.where(row // 2 == c, wide[:, :128], seen)
                seen = jnp.where(row // 2 == c + 1, wide[:, 128:], seen)
            raw[p % RAW, i, g] = seen

    def weigh(p, direct=False):
        high = stats[p, :, :, 0:128]
        top = jnp.max(high, 0)
        total = jnp.sum(stats[p, :, :, 128:256] * jnp.exp(high - top[None]), 0)
        share = jnp.exp(stats[p, me, :, 0:128] - top) / total
        for i in range(2):
            halves = []
            for g in range(2):
                scale = jnp.sum(jnp.where(lane == HALF * (2 * i + g) + row, share, 0.0), -1, keepdims=True)
                seen = raw[p % RAW, i, g] * scale
                halves.append(jnp.where(row % 2 == g, seen, pltpu.roll(seen, HEAD, 1)))
            seen = jnp.where(lane < HEAD, *halves).astype(BF16)
            if direct:
                parts[p - BUNCH * BUNCHES, me, i] = seen
            else:
                for g in range(2):
                    cut[p // BUNCH, 4 * (p % BUNCH) + 2 * i + g] = seen[8 * g : 8 * (g + 1)]

    def send_part(p):
        p = p - BUNCH * BUNCHES
        send(parts.at[p, me], part_send.at[p], part_recv.at[p])

    def send_cut(r):
        for peer in peers(me):
            pltpu.make_async_remote_copy(cut.at[r, peer], came.at[r, me], cut_send.at[r], cut_recv.at[r], device_id={"sp": peer}, device_id_type=MESH).start()

    def add_up(r):
        came[r, me] = cut[r, me]
        wait_peers(came.at[r], cut_recv.at[r])
        summed[r, me] = jnp.sum(came[r].astype(F32), 0).astype(BF16)
        send(summed.at[r, me], sum_send.at[r], sum_recv.at[r])

    def store(b, total):
        out_ref[b, 0:HALF, :] = total[:, :HEAD].astype(BF16)
        out_ref[b, HALF:HEADS, :] = pltpu.roll(total, HEAD, 1)[:, :HEAD].astype(BF16)

    def finish_bunch(r):
        wait_peers(summed.at[r], sum_recv.at[r])
        for i in range(2 * BUNCH):
            store(2 * BUNCH * r + i, jnp.concatenate([summed[r, 2 * i], summed[r, 2 * i + 1]], 0).astype(F32))

    def finish(p):
        p = p - BUNCH * BUNCHES
        wait_peers(parts.at[p], part_recv.at[p])
        for i in range(2):
            store(2 * (p + BUNCH * BUNCHES) + i, jnp.sum(parts[p, :, i].astype(F32), 0))

    q_copy = pltpu.make_async_copy(q_ref, qbuf, qsem)
    q_copy.start()
    for p in range(AHEAD):
        start(k_copy, p)
    barrier = pltpu.get_barrier_semaphore()
    for peer in peers(me):
        pl.semaphore_signal(barrier, inc=1, device_id={"sp": peer}, device_id_type=MESH)
    q_copy.wait()

    for p in range(LAG):
        wait(k_copy, p)
        start(k_copy, p + AHEAD)
        if p >= LAG - AHEAD:
            start(v_copy, p - LAG + AHEAD)
        scores(p)
    pl.semaphore_wait(barrier, DEV - 1)
    for p in range(LAG):
        send_stats(p)

    def both(p, more=True, due=(0,), direct=False):
        wait(k_copy, p + LAG)
        wait(v_copy, p)
        for d in due:
            wait_stats(p - d)
        if more:
            start(k_copy, p + LAG + AHEAD)
        start(v_copy, p + AHEAD)
        scores(p + LAG)
        for i in range(2):
            values(p, i)
        for d in due:
            weigh(p - d, direct)
        send_stats(p + LAG)

    both(0, due=())
    both(1, due=())
    both(2, due=(2, 1))
    both(3, due=(1, 0))
    send_cut(0)

    def middle(p, _):
        both(p)

        @pl.when(p % BUNCH == BUNCH - 1)
        def _():
            send_cut(p // BUNCH)

        @pl.when(p % BUNCH == 1)
        def _():
            add_up(p // BUNCH - 1)

        return 0

    turn = PAIRS - LAG - AHEAD
    lax.fori_loop(4, turn, middle, 0)
    for p in range(turn, turn + AHEAD):
        both(p, more=False, direct=p >= BUNCH * BUNCHES)
        if p >= BUNCH * BUNCHES:
            send_part(p)
        elif p % BUNCH == BUNCH - 1:
            send_cut(p // BUNCH)

    for p in range(PAIRS - LAG, PAIRS - 1):
        wait(v_copy, p)
        wait_stats(p)
        if p + AHEAD < PAIRS:
            start(v_copy, p + AHEAD)
        for i in range(2):
            values(p, i)
        weigh(p, True)
        send_part(p)
        if p == PAIRS - LAG:
            add_up(BUNCHES - 1)
    p = PAIRS - 1
    v_copy(2 * p).wait()
    values(p, 0)
    v_copy(2 * p + 1).wait()
    values(p, 1)
    wait_stats(p)
    weigh(p, True)
    send_part(p)

    for r in range(BUNCHES):
        finish_bunch(r)
        wait_peers(summed.at[r], sum_send.at[r])
        wait_peers(cut.at[r], cut_send.at[r])

    def drain(p, _):
        wait_peers(stats.at[p], stat_send.at[p])
        return 0

    lax.fori_loop(0, PAIRS, drain, 0)
    for p in range(PAIRS - DIRECT, PAIRS):
        finish(p)
    for p in range(DIRECT):
        wait_peers(parts.at[p], part_send.at[p])


def solution(mesh):
    def step(q, k, v):
        k, v = (x.transpose(0, 2, 3, 1).reshape(SEQ, HEADS * HEAD, RUN) for x in (k, v))
        return pl.pallas_call(
            kernel,
            out_shape=jax.ShapeDtypeStruct(q.shape, BF16),
            in_specs=[pl.BlockSpec(memory_space=pltpu.HBM)] * 3,
            out_specs=pl.BlockSpec(memory_space=pltpu.VMEM),
            scratch_shapes=[
                pltpu.VMEM(q.shape, BF16),
                pltpu.VMEM((SLOTS, HEADS * HEAD, RUN), BF16),
                pltpu.VMEM((SLOTS, HEADS * HEAD, RUN), BF16),
                pltpu.VMEM((SEQ, 2, HALF, RUN), BF16),
                pltpu.VMEM((RAW, 2, 2, HALF, 128), F32),
                pltpu.VMEM((PAIRS, DEV, 1, 256), F32),
                pltpu.VMEM((BUNCHES, DEV, 8, 128), BF16),
                pltpu.VMEM((BUNCHES, DEV, 8, 128), BF16),
                pltpu.VMEM((BUNCHES, DEV, 8, 128), BF16),
                pltpu.VMEM((DIRECT, DEV, 2, HALF, 128), BF16),
                pltpu.SemaphoreType.DMA,
                pltpu.SemaphoreType.DMA((SLOTS,)),
                pltpu.SemaphoreType.DMA((SLOTS,)),
                pltpu.SemaphoreType.DMA((PAIRS,)),
                pltpu.SemaphoreType.DMA((PAIRS,)),
                pltpu.SemaphoreType.DMA((BUNCHES,)),
                pltpu.SemaphoreType.DMA((BUNCHES,)),
                pltpu.SemaphoreType.DMA((BUNCHES,)),
                pltpu.SemaphoreType.DMA((BUNCHES,)),
                pltpu.SemaphoreType.DMA((DIRECT,)),
                pltpu.SemaphoreType.DMA((DIRECT,)),
            ],
            compiler_params=pltpu.CompilerParams(collective_id=0, has_side_effects=True, vmem_limit_bytes=50 * 2**20),
            name="attend",
        )(q, k, v)

    return jax.shard_map(
        step,
        mesh=mesh,
        in_specs=(P("dp", None, None), P("dp", "sp", None, None), P("dp", "sp", None, None)),
        out_specs=P("dp", None, None),
        check_vma=False,
    )
```

```python
import jax
import jax.numpy as jnp
from jax import lax
from jax.experimental import pallas as pl
from jax.experimental.pallas import tpu as pltpu
from jax.sharding import PartitionSpec as P

MESH = pl.DeviceIdType.MESH
BF16, F32 = jnp.bfloat16, jnp.float32

DEV = 16
SEQ = 32
PAIRS = SEQ // 2
HEADS = 32
HEAD = 64
RUN = 512
HALF = 16
ROWS = HALF * HEAD
LAG = 3
AHEAD = 2
SLOTS = 2 * (AHEAD + 1)
BUNCH = 4
BUNCHES = 3
DIRECT = PAIRS - BUNCH * BUNCHES
RAW = 3


def peers(me):
    bits = [(me // 2**i) % 2 for i in range(4)]
    for flip in (14, 15, 12, 10, 6, 13, 11, 7, 8, 4, 2, 9, 5, 3, 1):
        yield sum((1 - bit if flip >> i & 1 else bit) * 2**i for i, bit in enumerate(bits))


def kernel(q_ref, k_ref, v_ref, out_ref, qbuf, kbuf, vbuf, weights, raw, stats, cut, came, summed, parts, qsem, ksem, vsem, stat_send, stat_recv, cut_send, cut_recv, sum_send, sum_recv, part_send, part_recv):
    me = lax.axis_index("sp")
    row = lax.broadcasted_iota(jnp.int32, (HALF, 128), 0)
    lane = lax.broadcasted_iota(jnp.int32, (HALF, 128), 1)

    def k_copy(b):
        return pltpu.make_async_copy(k_ref.at[b], kbuf.at[b % SLOTS], ksem.at[b % SLOTS])

    def v_copy(b):
        return pltpu.make_async_copy(v_ref.at[b], vbuf.at[b % SLOTS], vsem.at[b % SLOTS])

    def start(copy, p):
        for i in range(2):
            copy(2 * p + i).start()

    def wait(copy, p):
        for i in range(2):
            copy(2 * p + i).wait()

    def send(ref, send_sem, recv_sem):
        for peer in peers(me):
            pltpu.make_async_remote_copy(ref, ref, send_sem, recv_sem, device_id={"sp": peer}, device_id_type=MESH).start()

    def wait_peers(ref, sem):
        some = ref.at[pl.ds(0, DEV - 1)]
        pltpu.make_async_copy(some, some, sem).wait()

    nothing = (jnp.zeros((HALF, 128), F32),) * 2

    def scores(p, i, found):
        highs, sums = found
        b = 2 * p + i
        for g in range(2):
            query = qbuf[b, HALF * g : HALF * (g + 1), :].astype(F32)
            query = jnp.concatenate([query, query], -1)
            query = jnp.where(lane // HEAD == row % 2, query, 0.0)
            query = jnp.concatenate([jnp.where(row // 2 == c, query, 0.0).astype(BF16) for c in range(HALF // 2)], -1)
            score = jnp.dot(query, kbuf[b % SLOTS, ROWS * g : ROWS * (g + 1), :], preferred_element_type=F32) * HEAD**-0.5
            high = jnp.max(score, -1, keepdims=True)
            weight = jnp.exp(score - high)
            weights[b, g] = weight.astype(BF16)
            here = lane // HALF == 2 * i + g
            highs = jnp.where(here, high, highs)
            sums = jnp.where(here, jnp.sum(weight, -1, keepdims=True), sums)
        return highs, sums

    def note(p, found):
        highs, sums = found
        mine = lane % HALF == row
        stats[p, me, :, 0:128] = jnp.sum(jnp.where(mine, highs, 0.0), 0, keepdims=True)
        stats[p, me, :, 128:256] = jnp.sum(jnp.where(mine, sums, 0.0), 0, keepdims=True)

    def send_stats(p):
        send(stats.at[p, me], stat_send.at[p], stat_recv.at[p])

    def wait_stats(p):
        wait_peers(stats.at[p], stat_recv.at[p])

    def values(p, i):
        b = 2 * p + i
        for g in range(2):
            seen = jnp.zeros((HALF, 128), F32)
            for c in range(0, HALF // 2, 2):
                first = ROWS * g + 128 * c
                wide = lax.dot_general(weights[b, g], vbuf[b % SLOTS, first : first + 256, :], (((1,), (1,)), ((), ())), preferred_element_type=F32)
                seen = jnp.where(row // 2 == c, wide[:, :128], seen)
                seen = jnp.where(row // 2 == c + 1, wide[:, 128:], seen)
            raw[p % RAW, i, g] = seen

    def weigh(p, direct=False):
        high = stats[p, :, :, 0:128]
        top = jnp.max(high, 0)
        total = jnp.sum(stats[p, :, :, 128:256] * jnp.exp(high - top[None]), 0)
        share = jnp.exp(stats[p, me, :, 0:128] - top) / total
        for i in range(2):
            halves = []
            for g in range(2):
                scale = jnp.sum(jnp.where(lane == HALF * (2 * i + g) + row, share, 0.0), -1, keepdims=True)
                seen = raw[p % RAW, i, g] * scale
                halves.append(jnp.where(row % 2 == g, seen, pltpu.roll(seen, HEAD, 1)))
            seen = jnp.where(lane < HEAD, *halves).astype(BF16)
            if direct:
                parts[p - BUNCH * BUNCHES, me, i] = seen
            else:
                for g in range(2):
                    cut[p // BUNCH, 4 * (p % BUNCH) + 2 * i + g] = seen[8 * g : 8 * (g + 1)]

    def send_part(p):
        p = p - BUNCH * BUNCHES
        send(parts.at[p, me], part_send.at[p], part_recv.at[p])

    def send_cut(r):
        for peer in peers(me):
            pltpu.make_async_remote_copy(cut.at[r, peer], came.at[r, me], cut_send.at[r], cut_recv.at[r], device_id={"sp": peer}, device_id_type=MESH).start()

    def add_up(r):
        came[r, me] = cut[r, me]
        wait_peers(came.at[r], cut_recv.at[r])
        summed[r, me] = jnp.sum(came[r].astype(F32), 0).astype(BF16)
        send(summed.at[r, me], sum_send.at[r], sum_recv.at[r])

    def store(b, total):
        out_ref[b, 0:HALF, :] = total[:, :HEAD].astype(BF16)
        out_ref[b, HALF:HEADS, :] = pltpu.roll(total, HEAD, 1)[:, :HEAD].astype(BF16)

    def finish_bunch(r):
        wait_peers(summed.at[r], sum_recv.at[r])
        for i in range(2 * BUNCH):
            store(2 * BUNCH * r + i, jnp.concatenate([summed[r, 2 * i], summed[r, 2 * i + 1]], 0).astype(F32))

    def finish(p):
        p = p - BUNCH * BUNCHES
        wait_peers(parts.at[p], part_recv.at[p])
        for i in range(2):
            store(2 * (p + BUNCH * BUNCHES) + i, jnp.sum(parts[p, :, i].astype(F32), 0))

    q_copy = pltpu.make_async_copy(q_ref, qbuf, qsem)
    q_copy.start()
    for p in range(AHEAD):
        start(k_copy, p)
    barrier = pltpu.get_barrier_semaphore()
    for peer in peers(me):
        pl.semaphore_signal(barrier, inc=1, device_id={"sp": peer}, device_id_type=MESH)
    q_copy.wait()

    for p in range(LAG):
        wait(k_copy, p)
        start(k_copy, p + AHEAD)
        if p >= LAG - AHEAD:
            start(v_copy, p - LAG + AHEAD)
        found = nothing
        for i in range(2):
            found = scores(p, i, found)
        note(p, found)
    pl.semaphore_wait(barrier, DEV - 1)
    for p in range(LAG):
        send_stats(p)

    def both(p, more=True, due=(1,), late=()):
        for d in due + late:
            wait_stats(p - d)
        found = nothing
        for i in range(2):
            k_copy(2 * (p + LAG) + i).wait()
            v_copy(2 * p + i).wait()
            if i == 0:
                for j in range(2):
                    if more:
                        k_copy(2 * (p + LAG + AHEAD) + j).start()
                    v_copy(2 * (p + AHEAD) + j).start()
            found = scores(p + LAG, i, found)
            values(p, i)
            if i == 0:
                for d in due:
                    weigh(p - d)
        note(p + LAG, found)
        for d in late:
            weigh(p - d)
        send_stats(p + LAG)

    both(0, due=())
    both(1, due=())
    both(2, due=(2, 1))
    both(3)

    def middle(p, _):
        both(p)

        @pl.when(p % BUNCH == 0)
        def _():
            send_cut(p // BUNCH - 1)

        @pl.when(p % BUNCH == 2)
        def _():
            add_up(p // BUNCH - 1)

        return 0

    turn = PAIRS - LAG - AHEAD
    lax.fori_loop(4, turn, middle, 0)
    both(turn, more=False, late=(0,))
    send_cut(BUNCHES - 1)
    both(turn + 1, more=False, due=())

    for p in range(PAIRS - LAG, PAIRS):
        wait(v_copy, p)
        wait_stats(p - 1)
        if p == PAIRS - 1:
            wait_stats(p)
        if p + AHEAD < PAIRS:
            start(v_copy, p + AHEAD)
        values(p, 0)
        weigh(p - 1, True)
        send_part(p - 1)
        values(p, 1)
        if p == PAIRS - 3:
            add_up(BUNCHES - 1)
    weigh(PAIRS - 1, True)
    send_part(PAIRS - 1)

    for r in range(BUNCHES):
        finish_bunch(r)
        wait_peers(summed.at[r], sum_send.at[r])
        wait_peers(cut.at[r], cut_send.at[r])

    def drain(p, _):
        wait_peers(stats.at[p], stat_send.at[p])
        return 0

    lax.fori_loop(0, PAIRS, drain, 0)
    for p in range(DIRECT):
        wait_peers(parts.at[p], part_send.at[p])
        finish(p + PAIRS - DIRECT)


def solution(mesh):
    def step(q, k, v):
        k, v = (x.transpose(0, 2, 3, 1).reshape(SEQ, HEADS * HEAD, RUN) for x in (k, v))
        q = pltpu.with_memory_space_constraint(q, pltpu.HBM)
        return pl.pallas_call(
            kernel,
            out_shape=jax.ShapeDtypeStruct(q.shape, BF16),
            in_specs=[pl.BlockSpec(memory_space=pltpu.HBM)] * 3,
            out_specs=pl.BlockSpec(memory_space=pltpu.VMEM),
            scratch_shapes=[
                pltpu.VMEM(q.shape, BF16),
                pltpu.VMEM((SLOTS, HEADS * HEAD, RUN), BF16),
                pltpu.VMEM((SLOTS, HEADS * HEAD, RUN), BF16),
                pltpu.VMEM((SEQ, 2, HALF, RUN), BF16),
                pltpu.VMEM((RAW, 2, 2, HALF, 128), F32),
                pltpu.VMEM((PAIRS, DEV, 1, 256), F32),
                pltpu.VMEM((BUNCHES, DEV, 8, 128), BF16),
                pltpu.VMEM((BUNCHES, DEV, 8, 128), BF16),
                pltpu.VMEM((BUNCHES, DEV, 8, 128), BF16),
                pltpu.VMEM((DIRECT, DEV, 2, HALF, 128), BF16),
                pltpu.SemaphoreType.DMA,
                pltpu.SemaphoreType.DMA((SLOTS,)),
                pltpu.SemaphoreType.DMA((SLOTS,)),
                pltpu.SemaphoreType.DMA((PAIRS,)),
                pltpu.SemaphoreType.DMA((PAIRS,)),
                pltpu.SemaphoreType.DMA((BUNCHES,)),
                pltpu.SemaphoreType.DMA((BUNCHES,)),
                pltpu.SemaphoreType.DMA((BUNCHES,)),
                pltpu.SemaphoreType.DMA((BUNCHES,)),
                pltpu.SemaphoreType.DMA((DIRECT,)),
                pltpu.SemaphoreType.DMA((DIRECT,)),
            ],
            compiler_params=pltpu.CompilerParams(collective_id=0, has_side_effects=True, vmem_limit_bytes=50 * 2**20),
            name="attend",
        )(q, k, v)

    return jax.shard_map(
        step,
        mesh=mesh,
        in_specs=(P("dp", None, None), P("dp", "sp", None, None), P("dp", "sp", None, None)),
        out_specs=P("dp", None, None),
        check_vma=False,
    )
```

```python
import jax
import jax.numpy as jnp
from jax import lax
from jax.experimental import pallas as pl
from jax.experimental.pallas import tpu as pltpu
from jax.sharding import PartitionSpec as P

MESH = pl.DeviceIdType.MESH
BF16, F32 = jnp.bfloat16, jnp.float32

DEV = 16
SEQ = 32
PAIRS = SEQ // 2
HEADS = 32
HEAD = 64
RUN = 512
HALF = 16
ROWS = HALF * HEAD
LAG = 3
AHEAD = 2
SLOTS = 2 * (AHEAD + 1)
BUNCH = 4
BUNCHES = 3
DIRECT = PAIRS - BUNCH * BUNCHES
RAW = 3


def peers(me):
    bits = [(me // 2**i) % 2 for i in range(4)]
    for flip in (14, 15, 12, 10, 6, 13, 11, 7, 8, 4, 2, 9, 5, 3, 1):
        yield sum((1 - bit if flip >> i & 1 else bit) * 2**i for i, bit in enumerate(bits))


def kernel(q_ref, k_ref, v_ref, out_ref, qbuf, kbuf, vbuf, weights, raw, stats, cut, came, summed, parts, qsem, ksem, vsem, stat_send, stat_recv, cut_send, cut_recv, sum_send, sum_recv, part_send, part_recv):
    me = lax.axis_index("sp")
    row = lax.broadcasted_iota(jnp.int32, (HALF, 128), 0)
    lane = lax.broadcasted_iota(jnp.int32, (HALF, 128), 1)

    def k_copy(b):
        return pltpu.make_async_copy(k_ref.at[b], kbuf.at[b % SLOTS], ksem.at[b % SLOTS])

    def v_copy(b):
        return pltpu.make_async_copy(v_ref.at[b], vbuf.at[b % SLOTS], vsem.at[b % SLOTS])

    def start(copy, p):
        for i in range(2):
            copy(2 * p + i).start()

    def wait(copy, p):
        for i in range(2):
            copy(2 * p + i).wait()

    def send(ref, send_sem, recv_sem):
        for peer in peers(me):
            pltpu.make_async_remote_copy(ref, ref, send_sem, recv_sem, device_id={"sp": peer}, device_id_type=MESH).start()

    def wait_peers(ref, sem):
        some = ref.at[pl.ds(0, DEV - 1)]
        pltpu.make_async_copy(some, some, sem).wait()

    nothing = (jnp.zeros((HALF, 128), F32),) * 2

    def scores(p, i, found):
        highs, sums = found
        b = 2 * p + i
        for g in range(2):
            query = qbuf[b, HALF * g : HALF * (g + 1), :].astype(F32)
            query = jnp.concatenate([query, query], -1)
            query = jnp.where(lane // HEAD == row % 2, query, 0.0)
            query = jnp.concatenate([jnp.where(row // 2 == c, query, 0.0).astype(BF16) for c in range(HALF // 2)], -1)
            score = jnp.dot(query, kbuf[b % SLOTS, ROWS * g : ROWS * (g + 1), :], preferred_element_type=F32) * HEAD**-0.5
            high = jnp.max(score, -1, keepdims=True)
            weight = jnp.exp(score - high)
            weights[b, g] = weight.astype(BF16)
            here = lane // HALF == 2 * i + g
            highs = jnp.where(here, high, highs)
            sums = jnp.where(here, jnp.sum(weight, -1, keepdims=True), sums)
        return highs, sums

    def note(p, found):
        highs, sums = found
        mine = lane % HALF == row
        stats[p, me, :, 0:128] = jnp.sum(jnp.where(mine, highs, 0.0), 0, keepdims=True)
        stats[p, me, :, 128:256] = jnp.sum(jnp.where(mine, sums, 0.0), 0, keepdims=True)

    def send_stats(p):
        send(stats.at[p, me], stat_send.at[p], stat_recv.at[p])

    def wait_stats(p):
        wait_peers(stats.at[p], stat_recv.at[p])

    def values(p, i):
        b = 2 * p + i
        for g in range(2):
            seen = jnp.zeros((HALF, 128), F32)
            for c in range(0, HALF // 2, 2):
                first = ROWS * g + 128 * c
                wide = lax.dot_general(weights[b, g], vbuf[b % SLOTS, first : first + 256, :], (((1,), (1,)), ((), ())), preferred_element_type=F32)
                seen = jnp.where(row // 2 == c, wide[:, :128], seen)
                seen = jnp.where(row // 2 == c + 1, wide[:, 128:], seen)
            raw[p % RAW, i, g] = seen

    def weigh(p, direct=False):
        high = stats[p, :, :, 0:128]
        top = jnp.max(high, 0)
        total = jnp.sum(stats[p, :, :, 128:256] * jnp.exp(high - top[None]), 0)
        share = jnp.exp(stats[p, me, :, 0:128] - top) / total
        for i in range(2):
            halves = []
            for g in range(2):
                scale = jnp.sum(jnp.where(lane == HALF * (2 * i + g) + row, share, 0.0), -1, keepdims=True)
                seen = raw[p % RAW, i, g] * scale
                halves.append(jnp.where(row % 2 == g, seen, pltpu.roll(seen, HEAD, 1)))
            seen = jnp.where(lane < HEAD, *halves).astype(BF16)
            if direct:
                parts[p - BUNCH * BUNCHES, me, i] = seen
            else:
                for g in range(2):
                    cut[p // BUNCH, 4 * (p % BUNCH) + 2 * i + g] = seen[8 * g : 8 * (g + 1)]

    def send_part(p):
        p = p - BUNCH * BUNCHES
        send(parts.at[p, me], part_send.at[p], part_recv.at[p])

    def send_cut(r):
        for peer in peers(me):
            pltpu.make_async_remote_copy(cut.at[r, peer], came.at[r, me], cut_send.at[r], cut_recv.at[r], device_id={"sp": peer}, device_id_type=MESH).start()

    def add_up(r):
        came[r, me] = cut[r, me]
        wait_peers(came.at[r], cut_recv.at[r])
        summed[r, me] = jnp.sum(came[r].astype(F32), 0).astype(BF16)
        send(summed.at[r, me], sum_send.at[r], sum_recv.at[r])

    def store(b, total):
        out_ref[b, 0:HALF, :] = total[:, :HEAD].astype(BF16)
        out_ref[b, HALF:HEADS, :] = pltpu.roll(total, HEAD, 1)[:, :HEAD].astype(BF16)

    def finish_bunch(r):
        wait_peers(summed.at[r], sum_recv.at[r])
        for i in range(2 * BUNCH):
            store(2 * BUNCH * r + i, jnp.concatenate([summed[r, 2 * i], summed[r, 2 * i + 1]], 0).astype(F32))

    def finish(p):
        p = p - BUNCH * BUNCHES
        wait_peers(parts.at[p], part_recv.at[p])
        for i in range(2):
            store(2 * (p + BUNCH * BUNCHES) + i, jnp.sum(parts[p, :, i].astype(F32), 0))

    q_copy = pltpu.make_async_copy(q_ref, qbuf, qsem)
    q_copy.start()
    for p in range(AHEAD):
        start(k_copy, p)
    barrier = pltpu.get_barrier_semaphore()
    for peer in peers(me):
        pl.semaphore_signal(barrier, inc=1, device_id={"sp": peer}, device_id_type=MESH)
    q_copy.wait()

    for p in range(LAG):
        wait(k_copy, p)
        start(k_copy, p + AHEAD)
        if p >= LAG - AHEAD:
            start(v_copy, p - LAG + AHEAD)
        found = nothing
        for i in range(2):
            found = scores(p, i, found)
        note(p, found)
    pl.semaphore_wait(barrier, DEV - 1)
    for p in range(LAG):
        send_stats(p)

    def both(p, more=True, due=(1,), late=()):
        for d in due + late:
            wait_stats(p - d)
        found = nothing
        for i in range(2):
            k_copy(2 * (p + LAG) + i).wait()
            v_copy(2 * p + i).wait()
            if i == 0:
                for j in range(2):
                    if more:
                        k_copy(2 * (p + LAG + AHEAD) + j).start()
                    v_copy(2 * (p + AHEAD) + j).start()
            found = scores(p + LAG, i, found)
            values(p, i)
            if i == 0:
                for d in due:
                    weigh(p - d)
        note(p + LAG, found)
        for d in late:
            weigh(p - d)
        send_stats(p + LAG)

    both(0, due=())
    both(1, due=())
    both(2, due=(2, 1))
    both(3)

    def middle(p, _):
        both(p)

        @pl.when(p % BUNCH == 0)
        def _():
            send_cut(p // BUNCH - 1)

        @pl.when(p % BUNCH == 2)
        def _():
            add_up(p // BUNCH - 1)

        return 0

    turn = PAIRS - LAG - AHEAD
    lax.fori_loop(4, turn, middle, 0)
    both(turn, more=False, late=(0,))
    send_cut(BUNCHES - 1)
    both(turn + 1, more=False, due=())

    for p in range(PAIRS - LAG, PAIRS):
        wait(v_copy, p)
        wait_stats(p - 1)
        if p + AHEAD < PAIRS:
            start(v_copy, p + AHEAD)
        values(p, 0)
        weigh(p - 1, True)
        send_part(p - 1)
        if p == PAIRS - 1:
            wait_stats(p)
        values(p, 1)
        if p == PAIRS - 3:
            add_up(BUNCHES - 1)
    weigh(PAIRS - 1, True)
    send_part(PAIRS - 1)

    for r in range(BUNCHES):
        finish_bunch(r)
        wait_peers(summed.at[r], sum_send.at[r])
        wait_peers(cut.at[r], cut_send.at[r])

    def drain(p, _):
        wait_peers(stats.at[p], stat_send.at[p])
        return 0

    lax.fori_loop(0, PAIRS, drain, 0)
    for p in range(DIRECT):
        wait_peers(parts.at[p], part_send.at[p])
        finish(p + PAIRS - DIRECT)


def solution(mesh):
    def step(q, k, v):
        k, v = (x.transpose(0, 2, 3, 1).reshape(SEQ, HEADS * HEAD, RUN) for x in (k, v))
        q = pltpu.with_memory_space_constraint(q, pltpu.HBM)
        return pl.pallas_call(
            kernel,
            out_shape=jax.ShapeDtypeStruct(q.shape, BF16),
            in_specs=[pl.BlockSpec(memory_space=pltpu.HBM)] * 3,
            out_specs=pl.BlockSpec(memory_space=pltpu.VMEM),
            scratch_shapes=[
                pltpu.VMEM(q.shape, BF16),
                pltpu.VMEM((SLOTS, HEADS * HEAD, RUN), BF16),
                pltpu.VMEM((SLOTS, HEADS * HEAD, RUN), BF16),
                pltpu.VMEM((SEQ, 2, HALF, RUN), BF16),
                pltpu.VMEM((RAW, 2, 2, HALF, 128), F32),
                pltpu.VMEM((PAIRS, DEV, 1, 256), F32),
                pltpu.VMEM((BUNCHES, DEV, 8, 128), BF16),
                pltpu.VMEM((BUNCHES, DEV, 8, 128), BF16),
                pltpu.VMEM((BUNCHES, DEV, 8, 128), BF16),
                pltpu.VMEM((DIRECT, DEV, 2, HALF, 128), BF16),
                pltpu.SemaphoreType.DMA,
                pltpu.SemaphoreType.DMA((SLOTS,)),
                pltpu.SemaphoreType.DMA((SLOTS,)),
                pltpu.SemaphoreType.DMA((PAIRS,)),
                pltpu.SemaphoreType.DMA((PAIRS,)),
                pltpu.SemaphoreType.DMA((BUNCHES,)),
                pltpu.SemaphoreType.DMA((BUNCHES,)),
                pltpu.SemaphoreType.DMA((BUNCHES,)),
                pltpu.SemaphoreType.DMA((BUNCHES,)),
                pltpu.SemaphoreType.DMA((DIRECT,)),
                pltpu.SemaphoreType.DMA((DIRECT,)),
            ],
            compiler_params=pltpu.CompilerParams(collective_id=0, has_side_effects=True, vmem_limit_bytes=50 * 2**20),
            name="attend",
        )(q, k, v)

    return jax.shard_map(
        step,
        mesh=mesh,
        in_specs=(P("dp", None, None), P("dp", "sp", None, None), P("dp", "sp", None, None)),
        out_specs=P("dp", None, None),
        check_vma=False,
    )
```
